256 devices in a mesh: trial: 2 (over z_hi), shard: 32 (over y, x, core), cols: 4 (over z_lo).
Axes of the slice: x: 4, y: 4, z: 8 (z_hi: 2, z_lo: 4; z = z_hi * 4 + z_lo), core: 2. Of those that a mesh axis runs over, the one named last changes fastest.
Arguments:
- train_gate: bfloat16 [4096, 8192], P(('trial', 'shard'), 'cols'), parts along dimension 0, may hold values from -0.125 to 0.125
- low_gate: bfloat16 [4096, 16], P(('trial', 'shard')), parts along dimension 0, may hold values from -0.125 to 0.125
- high_gate: bfloat16 [32, 8192], P('trial', 'cols'), parts along dimension 0, may hold values from -1.5 to 1.5
- train_up: bfloat16 [4096, 8192], P(('trial', 'shard'), 'cols'), parts along dimension 0, may hold values from -0.125 to 0.125
- low_up: bfloat16 [4096, 16], P(('trial', 'shard')), parts along dimension 0, may hold values from -0.125 to 0.125
- high_up: bfloat16 [32, 8192], P('trial', 'cols'), parts along dimension 0, may hold values from -1.5 to 1.5
- norm_train: float32 [4096], P(('trial', 'shard', 'cols')), parts along dimension 0, may hold values from 0.25 to 1.75
- norm_step: float32 [4096], P(('trial', 'shard', 'cols')), parts along dimension 0, may hold values from -0.3 to 0.3
Outputs:
- serve_gate: bfloat16 [16384, 2048], P(('trial', 'cols')), parts along dimension 0
- serve_up: bfloat16 [16384, 2048], P(('trial', 'cols')), parts along dimension 0
- serve_norm: bfloat16 [4096], P('trial'), parts along dimension 0
The draws below stay inside these ranges and needn't reach their ends.
There are 2 independent parts, one for each index of `trial`. The reference program is written for one: setup_inputs(seed, part) draws one part's arguments, and reference() takes and returns one part's arrays. A program takes and returns all parts, laid end to end along the dimension named above; each array names one. Nothing has to cross between parts.
All inputs are finite; a program needn't handle non-finite values.
Results may differ from the reference program's by a relative error of at most 0.001.
Values may be sent and summed in bfloat16 or wider, within the bound.
No kernel may reach another device: no remote copies, remote signals or barrier semaphores. Data moves between devices by JAX's collectives and lax.ppermute only.
A program may use at most 128 MiB of HBM per device.

```python
import jax
import jax.numpy as jnp

D_MODEL = 2048
D_INNER = 8192
RANK = 16


def steps_of(stream_key, extent, shards, low, largest):
    gain = 1.0
    for position, blocks in shards:
        heights = jax.random.uniform(jax.random.fold_in(jax.random.fold_in(stream_key, 6), position), (blocks,), jnp.float32, low / len(shards), largest / len(shards))
        gain = gain * jnp.repeat(jnp.exp(heights), extent[position] // blocks).reshape((-1,) + (1,) * (len(extent) - 1 - position))
    return gain


def centred(key, shape, width, reach, cuts=(), kind=jnp.bfloat16):
    loudness = steps_of(key, shape, cuts, -0.22, 0.18) if cuts else 1.0
    array = jax.random.normal(key, shape, jnp.float32) * width * loudness
    return jnp.minimum(jnp.maximum(array, -reach), reach).astype(kind)


def setup_inputs(seed: int = 0, part: int = 0) -> dict:
    key_list = jax.random.split(jax.random.key(seed), 9)
    part_splits = jax.random.split(jax.random.fold_in(key_list[8], part), 9)
    return {
        "train_gate": centred(part_splits[0], (D_MODEL, D_INNER), D_MODEL ** -0.5, 0.125, ((0, 32), (1, 4))),
        "low_gate": centred(part_splits[1], (D_MODEL, RANK), D_MODEL ** -0.5, 0.125, ((0, 32),)),
        "high_gate": centred(part_splits[2], (RANK, D_INNER), RANK ** -0.5, 1.5, ((1, 4),)),
        "train_up": centred(part_splits[3], (D_MODEL, D_INNER), D_MODEL ** -0.5, 0.125, ((0, 32), (1, 4))),
        "low_up": centred(part_splits[4], (D_MODEL, RANK), D_MODEL ** -0.5, 0.125, ((0, 32),)),
        "high_up": centred(part_splits[5], (RANK, D_INNER), RANK ** -0.5, 1.5, ((1, 4),)),
        "norm_train": jnp.clip(1.0 + 0.15 * jax.random.normal(part_splits[6], (D_MODEL,), jnp.float32), 0.25, 1.75),
        "norm_step": jnp.clip(jax.random.uniform(part_splits[7], (D_MODEL,), jnp.float32, -0.3, 0.3) * steps_of(part_splits[7], (D_MODEL,), ((0, 128),), -0.4, 0.0), -0.3, 0.3),
    }


mix_rate = 2.0


def reference(train_gate, low_gate, high_gate, train_up, low_up, high_up, norm_train, norm_step):
    fresh_gate = train_gate.astype(jnp.float32) + mix_rate * jnp.dot(low_gate, high_gate, preferred_element_type=jnp.float32)
    fresh_up = train_up.astype(jnp.float32) + mix_rate * jnp.dot(low_up, high_up, preferred_element_type=jnp.float32)
    serve_gate = fresh_gate.T.astype(jnp.bfloat16)
    serve_up = fresh_up.T.astype(jnp.bfloat16)
    serve_norm = (norm_train + norm_step).astype(jnp.bfloat16)
    return serve_gate, serve_up, serve_norm
```

```python
import jax
import jax.numpy as jnp
from jax import lax
from jax.experimental import pallas as pl
from jax.experimental.pallas import tpu as pltpu
from jax.sharding import Mesh
from jax.sharding import PartitionSpec as P


PLANE = ("y", "x", "core")
SIDE = 4
CHIPS = SIDE * SIDE
LANES = 128
MIX_RATE = 2.0
MIB = 1024 * 1024


def along(a, step):
    pairs = []
    for y in range(SIDE):
        for x in range(SIDE):
            pairs.append(((y * SIDE + x) * 2, (y * SIDE + (x + step) % SIDE) * 2))
            pairs.append(((y * SIDE + x) * 2 + 1, (((y + step) % SIDE) * SIDE + x) * 2 + 1))
    return lax.ppermute(a, PLANE, pairs)


def swap(a):
    return lax.ppermute(a, "core", [(0, 1), (1, 0)])


def from_col(a, step):
    return lax.ppermute(a, "cols", [((c + step) % 4, c) for c in range(4)])


def from_far(a):
    pairs = [
        (y * SIDE + x, (y + 2) % SIDE * SIDE + (x + 2) % SIDE) for y in range(SIDE) for x in range(SIDE)
    ]
    return lax.ppermute(a, ("y", "x"), pairs)


def vmem():
    return pl.BlockSpec(memory_space=pltpu.VMEM)


def load_body(*refs):
    ins, outs, sems = refs[:8], refs[8:16], refs[16]
    copies = [pltpu.make_async_copy(a, b, sems.at[i]) for i, (a, b) in enumerate(zip(ins, outs))]
    for c in copies:
        c.start()
    for c in copies:
        c.wait()


def load(*arrays):
    return pl.pallas_call(
        load_body,
        out_shape=tuple(pltpu.VMEM(a.shape, a.dtype) for a in arrays),
        in_specs=[pl.BlockSpec(memory_space=pltpu.HBM)] * len(arrays),
        out_specs=tuple(vmem() for _ in arrays),
        scratch_shapes=[pltpu.SemaphoreType.DMA((len(arrays),))],
        compiler_params=pltpu.CompilerParams(vmem_limit_bytes=60 * 1024 * 1024),
        name="load",
    )(*arrays)


def merge_body(
    gate, up, gate2, up2, low_g, low_u, low_g2, low_u2, high_g, high_u,
    norm, step, norm2, step2, mine, table,
):
    core = lax.axis_index("core")
    first = core == 0
    half = gate.shape[1] // 2

    def write(start):
        for i, (w, w2, low, low2, high) in enumerate(
            ((gate, gate2, low_g, low_g2, high_g), (up, up2, low_u, low_u2, high_u))
        ):
            a = w[:, start : start + half].astype(jnp.float32)
            b = w2[:, start : start + half].astype(jnp.float32)
            rows = jnp.concatenate([jnp.where(first, a, b), jnp.where(first, b, a)], axis=0)
            la, lb = low[...].astype(jnp.float32), low2[...].astype(jnp.float32)
            lows = jnp.concatenate([jnp.where(first, la, lb), jnp.where(first, lb, la)], axis=1)
            delta = lax.dot_general(
                lows.astype(jnp.bfloat16),
                high[:, start : start + half],
                (((0,), (0,)), ((), ())),
                preferred_element_type=jnp.float32,
            )
            mine[i * half : (i + 1) * half] = (rows + MIX_RATE * delta).T.astype(jnp.bfloat16)

    @pl.when(first)
    def _():
        write(0)

    @pl.when(jnp.logical_not(first))
    def _():
        write(half)

    def spread(a, b, c):
        wide = jnp.concatenate([a[...] + b[...], jnp.zeros((1, LANES - 16), jnp.float32)], axis=1)
        return pltpu.roll(jnp.broadcast_to(wide, (CHIPS, LANES)), c * 64 + 16 * lax.axis_index("cols"), 1)

    gains = spread(norm, step, core) + spread(norm2, step2, 1 - core)
    chip = lax.axis_index("y") * SIDE + lax.axis_index("x")
    here = lax.broadcasted_iota(jnp.int32, (CHIPS, LANES), 0) == chip
    table[...] = jnp.where(here, gains, 0.0).astype(jnp.bfloat16)


def merge(*arrays):
    width = arrays[0].shape[1]
    return pl.pallas_call(
        merge_body,
        out_shape=(
            pltpu.VMEM((width, LANES), jnp.bfloat16),
            pltpu.VMEM((CHIPS, LANES), jnp.bfloat16),
        ),
        in_specs=[vmem()] * len(arrays),
        out_specs=(vmem(), vmem()),
        compiler_params=pltpu.CompilerParams(vmem_limit_bytes=8 * MIB),
        name="merge",
    )(*arrays)


def union(first, *others):
    for t in others:
        first = jnp.where(first != 0, first, t)
    return first


def place(pieces, given, tables=()):
    arrays = []
    for p in pieces:
        if not any(p[0] is a for a in arrays):
            arrays.append(p[0])
    slots = [next(i for i, a in enumerate(arrays) if a is p[0]) for p in pieces]
    n, given, tables = len(arrays), list(given), list(tables)
    width = CHIPS * LANES
    half = width // 2

    def body(*refs):
        ins, parts = refs[:n], refs[n + len(given) : n + len(given) + len(tables)]
        gate, up, *gains, sem = refs[n + len(given) + len(tables) :]
        core, x, y = lax.axis_index("core"), lax.axis_index("x"), lax.axis_index("y")
        copies = []
        for slot, (_, halves, partner, main, da, db) in zip(slots, pieces):
            c = 1 - core if partner else core
            stream = c if main else 1 - c
            px = lax.rem(x + jnp.where(c == 0, da, db) + SIDE, SIDE)
            py = lax.rem(y + jnp.where(c == 0, db, da) + SIDE, SIDE)
            col = pl.multiple_of((py * SIDE + px) * LANES, LANES)
            row = pl.multiple_of(stream * half, half)
            for h, start in halves.items():
                copies.append(
                    pltpu.make_async_copy(
                        ins[slot].at[pl.ds(start, half)],
                        (gate, up)[h].at[pl.ds(row, half), pl.ds(col, LANES)],
                        sem,
                    )
                )
        for c in copies:
            c.start()
        if gains:
            whole = [t[t.shape[0] - CHIPS :, :].astype(jnp.float32) for t in parts]
            gains[0][...] = union(*whole).astype(jnp.bfloat16)
        for c in copies:
            c.wait()

    anyspace = pl.BlockSpec(memory_space=pl.ANY)
    big = jax.ShapeDtypeStruct((width, width), jnp.bfloat16)
    small = [jax.ShapeDtypeStruct((CHIPS, LANES), jnp.bfloat16)] if tables else []
    return pl.pallas_call(
        body,
        out_shape=(big, big, *small),
        in_specs=[vmem()] * n + [anyspace] * len(given) + [vmem()] * len(tables),
        out_specs=(anyspace, anyspace, *[vmem() for _ in small]),
        scratch_shapes=[pltpu.SemaphoreType.DMA],
        input_output_aliases={n: 0, n + 1: 1} if given else {},
        compiler_params=pltpu.CompilerParams(vmem_limit_bytes=8 * MIB),
    )(*arrays, *given, *tables)


def steps(train_gate, low_gate, high_gate, train_up, low_up, high_up, norm_train, norm_step):
    low_g, low_u = low_gate.T, low_up.T
    norm, step = norm_train.reshape(1, -1), norm_step.reshape(1, -1)
    own = (train_gate, train_up, low_g, low_u, norm, step)
    gate2, up2, low_g2, low_u2, norm2, step2 = (swap(a) for a in own)
    gate, up, low_g, low_u, high_g, high_u, norm, step = load(
        train_gate, train_up, low_g, low_u, high_gate, high_up, norm, step
    )
    mine, table = merge(
        gate, up, gate2, up2, low_g, low_u, low_g2, low_u2, high_g, high_u, norm, step, norm2, step2
    )
    half = mine.shape[0] // 2

    other = swap(mine)
    p_l, p_r = along(mine, 1), along(mine, -1)
    q_l, q_r = along(other, 1), along(other, -1)
    table = union(table, *(from_col(table, s) for s in (1, 2, 3)))
    sp_l, sp_r = swap(p_l), swap(p_r)
    f_0 = along(jnp.concatenate([p_l[:half], table]), 1)
    f_1 = along(jnp.concatenate([p_r[half:], table]), -1)
    far = from_far(table)
    both = jnp.concatenate([sp_l, sp_r])
    s_l, s_r = along(both, 1), along(both, -1)
    sq_l, sq_r = swap(q_l), swap(q_r)
    sf_0, sf_1 = swap(f_0), swap(f_1)
    table = union(table, f_0[half:], f_1[half:], sf_0[half:], sf_1[half:])
    opp = jnp.concatenate([sf_0[:half], sf_1[:half], table])
    t_l, t_r = along(opp, 1), along(opp, -1)
    v_0 = along(jnp.concatenate([q_l[:half], s_l[:half], s_l[2 * half : 3 * half]]), 1)
    v_1 = along(jnp.concatenate([q_r[half:], s_r[half : 2 * half], s_r[3 * half :]]), -1)
    ss_l, ss_r = swap(s_l), swap(s_r)
    table = union(table, t_l[2 * half :], t_r[2 * half :])
    w_0 = along(jnp.concatenate([t_l[:half], table]), 1)
    w_1 = along(jnp.concatenate([t_r[half : 2 * half], table]), -1)
    st_l, st_r = swap(t_l), swap(t_r)
    sv_0, sv_1 = swap(v_0), swap(v_1)
    sw_0, sw_1 = swap(w_0), swap(w_1)

    whole = {0: 0, 1: half}

    def ends(l, r, partner, main, db):
        return [(l, whole, partner, main, -1, db), (r, whole, partner, main, 1, db)]

    def halves(a, b, partner, main, db, at=0):
        return [(a, {0: at}, partner, main, 2, db), (b, {1: at}, partner, main, 2, db)]

    pieces = [(mine, whole, False, True, 0, 0), (other, whole, False, False, 0, 0)]
    pieces += ends(p_l, p_r, False, True, 0) + ends(sp_l, sp_r, True, True, 0)
    pieces += halves(f_0, f_1, False, True, 0) + halves(sf_0, sf_1, True, True, 0)
    pieces += ends(q_l, q_r, False, False, 0) + ends(sq_l, sq_r, True, False, 0)
    outs = place(pieces, ())
    pieces = ends(t_l, t_r, False, False, 2)
    for l, r, partner in ((s_l, s_r, False), (ss_l, ss_r, True)):
        for at, db in ((0, -1), (2 * half, 1)):
            rows = {0: at, 1: at + half}
            pieces += [(l, rows, partner, False, -1, db), (r, rows, partner, False, 1, db)]
    outs = place(pieces, outs)

    def thirds(a, b, partner):
        return [p for i, db in enumerate((0, -1, 1)) for p in halves(a, b, partner, False, db, i * half)]

    outs = place(ends(st_l, st_r, True, False, 2) + thirds(v_0, v_1, False), outs)
    outs = place(thirds(sv_0, sv_1, True) + halves(w_0, w_1, False, False, 2), outs)
    pieces = halves(sw_0, sw_1, True, False, 2)
    serve_gate, serve_up, gains = place(pieces, outs, tables=(table, w_0, w_1, sw_0, sw_1, far))
    return serve_gate, serve_up, gains.reshape(-1)


def solution(mesh):
    finer = Mesh(
        mesh.devices.reshape(mesh.shape["trial"], SIDE, SIDE, 2, mesh.shape["cols"]),
        ("trial", *PLANE, "cols"),
    )
    rows = ("trial", *PLANE)
    weights = (P(rows, "cols"), P(rows, None), P("trial", "cols"))
    in_specs = weights + weights + (P((*rows, "cols")),) * 2
    out_specs = (P(("trial", "cols"), None), P(("trial", "cols"), None), P("trial"))
    return jax.shard_map(steps, mesh=finer, in_specs=in_specs, out_specs=out_specs, check_vma=False)
```
